16 devices in a mesh: dp: 2 (over y, z), ep: 8 (over x, core).
Axes of the slice: x: 4, y: 2, z: 1, core: 2. Of those that a mesh axis runs over, the one named last changes fastest.
The devices are a block of a 4x4x8 slice.
Arguments:
- x: bfloat16 [2, 8, 256, 5120], P('dp', 'ep'), parts along dimension 0
- expert: int32 [2, 8, 256, 8], P('dp', 'ep'), parts along dimension 0
- slot: int32 [2, 8, 256, 8], P('dp', 'ep'), parts along dimension 0
- gate: float32 [2, 8, 256, 8], P('dp', 'ep'), parts along dimension 0
- w_gate: bfloat16 [40, 5120, 1536], P('ep')
- w_up: bfloat16 [40, 5120, 1536], P('ep')
- w_down: bfloat16 [40, 1536, 5120], P('ep')
- s_gate: bfloat16 [5120, 1536], replicated
- s_up: bfloat16 [5120, 1536], replicated
- s_down: bfloat16 [1536, 5120], replicated
Outputs:
- y: bfloat16 [2, 8, 256, 5120], P('dp', 'ep'), parts along dimension 0
There are 2 independent parts. The reference program is written for one: setup_inputs(seed, part) draws one part's arguments, and reference() takes and returns one part's arrays. A program takes and returns all parts, laid end to end along the dimension named above; an argument that names none is the same for every part.
All inputs are finite; a program needn't handle non-finite values.
Results may differ from the reference program's by a relative error of at most 0.009.
Values are sent between devices in bfloat16 or wider.
A program may use at most 768 MiB of HBM per device.

```python
import jax
import jax.numpy as jnp

MEMBERS = 8
TOKENS = 256
D = 5120
FF = 1536
TOP = 8
EXPERTS = 40
SHARED_FF = 1536
SLOTS = 5 * TOKENS * TOP // (4 * EXPERTS)


def setup_inputs(seed: int = 0, part: int = 0) -> dict:
    own, k1, k2, k3, k4, k5, k6 = jax.random.split(jax.random.key(seed), 7)
    kx, ke, kl, kg = jax.random.split(jax.random.fold_in(own, part), 4)
    devices = (1, MEMBERS)
    place = jax.random.permutation(kl, jnp.arange(EXPERTS, dtype=jnp.uint32))
    slow = ((EXPERTS + (9 * place) % EXPERTS) << ((9 * place) // EXPERTS)) // EXPERTS
    wait = (jax.random.bits(ke, (*devices, TOKENS, EXPERTS), jnp.uint32) >> 10) * slow
    expert = jnp.argsort(wait, axis=-1)[..., :TOP].astype(jnp.int32)
    chosen = jax.nn.one_hot(expert, EXPERTS, dtype=jnp.int32)
    in_line = jnp.cumsum(chosen.reshape(*devices, TOKENS * TOP, EXPERTS), axis=2) - 1
    slot = jnp.sum(in_line.reshape(chosen.shape) * chosen, axis=-1)

    def one(key, rows, columns):
        return (jax.random.normal(key, (rows, columns), jnp.float32) * rows**-0.5).astype(jnp.bfloat16)

    def weights(key, rows, columns):
        return jax.lax.map(lambda k: one(k, rows, columns), jax.random.split(key, EXPERTS))

    return {
        "x": jax.random.normal(kx, (*devices, TOKENS, D), jnp.float32).astype(jnp.bfloat16),
        "expert": expert,
        "slot": slot,
        "gate": jax.nn.softmax(jax.random.normal(kg, expert.shape, jnp.float32)),
        "w_gate": weights(k1, D, FF),
        "w_up": weights(k2, D, FF),
        "w_down": weights(k3, FF, D),
        "s_gate": one(k4, D, SHARED_FF),
        "s_up": one(k5, D, SHARED_FF),
        "s_down": one(k6, SHARED_FF, D),
    }


def einsum(form, a, b):
    return jnp.einsum(form, a.astype(jnp.float32), b.astype(jnp.float32))


def for_all(x, s_gate, s_up, s_down):
    h = jax.nn.silu(einsum("...d,df->...f", x, s_gate)) * einsum("...d,df->...f", x, s_up)
    return einsum("...f,fd->...d", h.astype(jnp.bfloat16), s_down)


def reference(x, expert, slot, gate, w_gate, w_up, w_down, s_gate, s_up, s_down):
    to_expert = jax.nn.one_hot(expert, EXPERTS, dtype=jnp.bfloat16)
    to_slot = jax.nn.one_hot(slot, SLOTS, dtype=jnp.bfloat16)
    weighted = to_expert * gate[..., None].astype(jnp.bfloat16)
    dispatch = einsum("abtke,abtkc->abtec", to_expert, to_slot).astype(jnp.bfloat16)
    combine = einsum("abtke,abtkc->abtec", weighted, to_slot).astype(jnp.bfloat16)
    z = einsum("abtec,abtd->aebcd", dispatch, x).astype(jnp.bfloat16)
    h = jax.nn.silu(einsum("aebcd,edf->aebcf", z, w_gate))
    h = (h * einsum("aebcd,edf->aebcf", z, w_up)).astype(jnp.bfloat16)
    out = einsum("aebcf,efd->aebcd", h, w_down).astype(jnp.bfloat16)
    y = einsum("abtec,aebcd->abtd", combine, out)
    return (y + for_all(x, s_gate, s_up, s_down)).astype(jnp.bfloat16)
```

```python
import jax
import jax.numpy as jnp
from jax import lax
from jax.sharding import PartitionSpec as P

F32, BF16 = jnp.float32, jnp.bfloat16


def dot(form, a, b):
    return jnp.einsum(form, a, b, preferred_element_type=F32)


def solution(mesh):
    n = mesh.shape["ep"]

    def body(x, expert, slot, gate, w_gate, w_up, w_down, s_gate, s_up, s_down):
        x, expert, slot, gate = x[0, 0], expert[0, 0], slot[0, 0], gate[0, 0]
        (tokens, top), local = expert.shape, w_gate.shape[0]
        d, ff = w_gate.shape[1:]
        experts = local * n
        slots = 5 * tokens * top // (4 * experts)
        first = lax.axis_index("ep") * local
        meta = jnp.stack([expert.astype(F32), jnp.minimum(slot, slots).astype(F32), gate.astype(BF16).astype(F32)])
        meta = lax.all_gather(meta, "ep")
        xs = lax.all_gather(x, "ep")
        e = meta[:, 0].astype(jnp.int32) - first
        s = meta[:, 1].astype(jnp.int32)
        g = meta[:, 2].astype(BF16)
        ok = (e >= 0) & (e < local) & (s < slots)
        row = jnp.where(ok, e * slots + s, -1)
        hot = jax.nn.one_hot(row, local * slots, dtype=BF16)
        dispatch = jnp.sum(hot, axis=2).astype(BF16)
        combine = jnp.sum(hot * g[..., None], axis=2).astype(BF16)
        z = dot("btr,btd->brd", dispatch, xs).astype(BF16)
        z = z.reshape(n, local, slots, d)
        h = jax.nn.silu(dot("becd,edf->ebcf", z, w_gate))
        h = (h * dot("becd,edf->ebcf", z, w_up)).astype(BF16)
        hs = jax.nn.silu(dot("td,df->tf", x, s_gate))
        hs = (hs * dot("td,df->tf", x, s_up)).astype(BF16)
        shared = dot("tf,fd->td", hs, s_down)
        parts, w = [], d // 4
        for i in range(0, d, w):
            out = dot("ebcf,efd->becd", h, w_down[:, :, i : i + w]).astype(BF16)
            out = out.reshape(n, local * slots, w)
            y = dot("btr,brd->btd", combine, out).astype(BF16)
            parts.append(lax.psum_scatter(y, "ep", scatter_dimension=0, tiled=False))
        y = jnp.concatenate(parts, axis=-1).astype(F32)
        return (y + shared).astype(BF16)[None, None]

    a, e, r = P("dp", "ep", None, None), P("ep", None, None), P(None, None)
    return jax.shard_map(body, mesh=mesh, in_specs=(a, a, a, a, e, e, e, r, r, r), out_specs=a, check_vma=False)
```

```python
import functools

import jax
import jax.numpy as jnp
from jax import lax
from jax.experimental import pallas as pl
from jax.experimental.pallas import tpu as pltpu
from jax.sharding import PartitionSpec as P

F32, BF16 = jnp.float32, jnp.bfloat16
MESH = pl.DeviceIdType.MESH
ANY = pl.BlockSpec(memory_space=pl.ANY)
VM = pl.BlockSpec(memory_space=pltpu.VMEM)
WIDTH = 512
RING = 3


def mm(a, b):
    return jnp.dot(a, b, preferred_element_type=F32)


def silu(v):
    return v * (1.0 / (1.0 + jnp.exp(-v)))


def places(n):
    me = lax.axis_index("ep")
    chips = n // 2
    chip, core = lax.div(me, 2), lax.rem(me, 2)
    right, left = lax.rem(chip + 1, chips), lax.rem(chip + chips - 1, chips)
    across = lax.rem(chip + 2, chips)
    return me, chips, chip, core, right, left, across


def send(src, dst, send_sem, recv_sem, device):
    pltpu.make_async_remote_copy(
        src_ref=src, dst_ref=dst, send_sem=send_sem, recv_sem=recv_sem, device_id={"ep": device}, device_id_type=MESH
    ).start()


def wait(ref, sem):
    pltpu.make_async_copy(ref, ref, sem).wait()


def up_kernel(n, local, slots, x, mt, wg, wu, sg, su, h, hs, gt, xg, acc_g, acc_u, wbuf, xv, z, dm, gm, meta, hst,
              meta_send, meta_recv, own_send, fwd_send, pass_send, recv_l, recv_r, recv_a, recv_b, recv_p,
              wsem, xsem, ldsem, osem):
    me, chips, chip, core, right, left, across = places(n)
    dev_r, dev_l, dev_p = right * 2 + core, left * 2 + core, chip * 2 + 1 - core
    tokens, d = x.shape
    ff = sg.shape[1]
    chunks = d // WIDTH
    half = tokens // 2
    rows = n * slots
    top = mt.shape[0] // 4

    def cols(c):
        return pl.ds(pl.multiple_of(c * WIDTH, WIDTH), WIDTH)

    def fetch_shared(c):
        slot = lax.rem(c, RING)
        pltpu.make_async_copy(sg.at[cols(c), :], wbuf.at[slot, 0], wsem.at[slot]).start()
        pltpu.make_async_copy(su.at[cols(c), :], wbuf.at[slot, 1], wsem.at[slot]).start()

    def fetch(t):
        slot = lax.rem(t + chunks, RING)
        c, e = lax.div(t, local), lax.rem(t, local)
        pltpu.make_async_copy(wg.at[e, cols(c), :], wbuf.at[slot, 0], wsem.at[slot]).start()
        pltpu.make_async_copy(wu.at[e, cols(c), :], wbuf.at[slot, 1], wsem.at[slot]).start()

    fetch_shared(0)
    fetch_shared(1)

    def piece(c):
        return xv.at[c // 8, (c % 8) // 4, c % 4]

    for c in range(chunks):
        pltpu.make_async_copy(x.at[:, cols(c)], piece(c), xsem.at[c]).start()

    barrier = pltpu.get_barrier_semaphore()
    for r in range(1, n):
        pl.semaphore_signal(barrier, inc=1, device_id={"ep": lax.rem(me + r, n)}, device_id_type=MESH)
    pl.semaphore_wait(barrier, n - 1)

    mine = core * chips + chip

    def own(c):
        src, dst = x.at[:, cols(c)], xg.at[c, core, chip]
        send(src, dst, own_send.at[0], recv_l.at[c], dev_r)
        send(src, dst, own_send.at[1], recv_r.at[c], dev_l)
        send(src, dst, own_send.at[2], recv_p.at[c], dev_p)

    def forward(c):
        piece_l, piece_r = xg.at[c, core, left], xg.at[c, core, right]
        wait(piece_l, recv_l.at[c])
        upper = piece_l.at[pl.ds(0, half)]
        send(upper, upper, fwd_send.at[0], recv_a.at[c], dev_r)
        wait(piece_r, recv_r.at[c])
        lower = piece_r.at[pl.ds(half, half)]
        send(lower, lower, fwd_send.at[1], recv_b.at[c], dev_l)
        send(piece_l, piece_l, pass_send.at[0], recv_p.at[c], dev_p)
        send(piece_r, piece_r, pass_send.at[1], recv_p.at[c], dev_p)

    def last_hop(c):
        piece_o = xg.at[c, core, across]
        wait(piece_o.at[pl.ds(0, half)], recv_a.at[c])
        wait(piece_o.at[pl.ds(half, half)], recv_b.at[c])
        send(piece_o, piece_o, pass_send.at[2], recv_p.at[c], dev_p)

    def load(c):
        slot = lax.rem(c, 2)
        wait(xg.at[c, 1 - core], recv_p.at[c])
        pltpu.make_async_copy(xg.at[c, 1 - core], xv.at[slot, 1 - core], ldsem.at[slot]).start()
        pltpu.make_async_copy(x.at[:, cols(c)], xv.at[slot, core, chip], ldsem.at[slot]).start()
        for other in (left, right, across):
            pltpu.make_async_copy(xg.at[c, core, other], xv.at[slot, core, other], ldsem.at[slot]).start()

    own(0)
    for r in range(1, n):
        send(mt, meta.at[mine], meta_send.at[r], meta_recv.at[mine], lax.rem(me + r, n))
    meta[mine] = mt[...]

    tiles = [(i, min(i + WIDTH, ff)) for i in range(0, ff, WIDTH)]

    def shared_step(c):
        slot = c % RING
        wait(wbuf.at[slot], wsem.at[slot])
        if c + 2 < chunks:
            fetch_shared(c + 2)
        else:
            fetch(jnp.int32(c + 2 - chunks))
        wait(piece(c), xsem.at[c])
        xc = piece(c)[...]
        for lo, hi in tiles:
            for k, acc in ((0, acc_g), (1, acc_u)):
                v = mm(xc, wbuf[slot, k, :, lo:hi])
                acc[0, :tokens, lo:hi] = v if c == 0 else acc[0, :tokens, lo:hi] + v

    for c in range(chunks):
        if c == chunks - 2:
            forward(0)
            own(1)
        shared_step(c)
    hst[0, :tokens] = (silu(acc_g[0, :tokens]) * acc_u[0, :tokens]).astype(BF16)
    pltpu.make_async_copy(hst.at[0, pl.ds(0, tokens)], hs, osem.at[0]).start()

    for r in range(1, n):
        src = lax.rem(me + r, n)
        q = lax.rem(src, 2) * chips + lax.div(src, 2)
        wait(meta.at[q], meta_recv.at[q])
    first = (me * local).astype(F32)

    @pl.loop(0, n)
    def _(q):
        m = meta[q].astype(F32)
        e, s, g = m[0:top], m[top : 2 * top], m[2 * top : 3 * top]
        ok = (e >= first) & (e < first + local) & (s < slots)
        key = jnp.where(ok, (e - first) * slots + s, -1.0)
        for i in range(local):
            row = lax.broadcasted_iota(jnp.int32, (slots, tokens), 0).astype(F32) + float(i * slots)
            hot = jnp.zeros((slots, tokens), F32)
            weight = jnp.zeros((slots, tokens), F32)
            for k in range(top):
                hit = row == key[k : k + 1]
                hot = jnp.where(hit, 1.0, hot)
                weight = jnp.where(hit, g[k : k + 1], weight)
            dm[q, i * slots : (i + 1) * slots] = hot.astype(BF16)
            gm[q, i * slots : (i + 1) * slots] = weight.astype(BF16)

    last_hop(0)
    pltpu.make_async_copy(gm, gt, osem.at[1]).start()
    wait(hs, osem.at[0])
    load(0)

    def dispatch(c):
        slot = lax.rem(c, 2)
        wait(xv.at[slot], ldsem.at[slot])
        for q in range(n):
            v = mm(dm[q], xv[slot, q // chips, q % chips]).astype(BF16)
            for i in range(local):
                z[i, q * slots : (q + 1) * slots] = v[i * slots : (i + 1) * slots]

    steps = chunks * local

    @pl.loop(0, steps - local)
    def _(t):
        c, e = lax.div(t, local), lax.rem(t, local)
        slot = lax.rem(t + chunks, RING)

        @pl.when(e == 0)
        def _():
            dispatch(c)

        @pl.when(e == 1)
        def _():
            forward(c + 1)

            @pl.when(c + 2 < chunks)
            def _():
                own(c + 2)

        @pl.when(e == 3)
        def _():
            last_hop(c + 1)

        @pl.when(e == 4)
        def _():
            load(c + 1)

        wait(wbuf.at[slot], wsem.at[slot])
        fetch(t + 2)
        ze = z[e]
        for lo, hi in tiles:
            for k, acc in ((0, acc_g), (1, acc_u)):
                v = mm(ze, wbuf[slot, k, :, lo:hi])
                acc[e, :, lo:hi] = jnp.where(c == 0, 0.0, acc[e, :, lo:hi]) + v

    dispatch(jnp.int32(chunks - 1))

    @pl.loop(0, local)
    def _(e):
        t = steps - local + e
        slot = lax.rem(t + chunks, RING)
        wait(wbuf.at[slot], wsem.at[slot])

        @pl.when(e + 2 < local)
        def _():
            fetch(t + 2)

        to = lax.rem(e, 2)

        @pl.when(e >= 2)
        def _():
            wait(hst.at[to], osem.at[2 + to])

        ze = z[e]
        for lo, hi in tiles:
            g = acc_g[e, :, lo:hi] + mm(ze, wbuf[slot, 0, :, lo:hi])
            u = acc_u[e, :, lo:hi] + mm(ze, wbuf[slot, 1, :, lo:hi])
            hst[to, :, lo:hi] = (silu(g) * u).astype(BF16)
        pltpu.make_async_copy(hst.at[to], h.at[e], osem.at[2 + to]).start()

    for to in range(2):
        wait(hst.at[to], osem.at[2 + to])
    wait(gm, osem.at[1])
    for i in range(3):
        wait(x, own_send.at[i])
        wait(x, pass_send.at[i])
    for i in range(2):
        wait(x.at[pl.ds(0, half)], fwd_send.at[i])
    for r in range(1, n):
        wait(mt, meta_send.at[r])


def up(n, slots, x, mt, wg, wu, sg, su):
    tokens, d = x.shape
    local, _, ff = wg.shape
    chunks, rows, chips = d // WIDTH, n * slots, n // 2
    dma = pltpu.SemaphoreType.DMA
    flops = 2 * (rows * local + tokens) * d * ff * 2
    moved = 2 * (2 * local + 2) * d * ff
    return pl.pallas_call(
        functools.partial(up_kernel, n, local, slots),
        out_shape=[
            jax.ShapeDtypeStruct((local, rows, ff), BF16),
            jax.ShapeDtypeStruct((tokens, ff), BF16),
            jax.ShapeDtypeStruct((n, local * slots, tokens), BF16),
            jax.ShapeDtypeStruct((chunks, 2, chips, tokens, WIDTH), BF16),
        ],
        in_specs=[ANY, VM, ANY, ANY, ANY, ANY],
        out_specs=[ANY] * 4,
        scratch_shapes=[
            pltpu.VMEM((local, rows, ff), F32),
            pltpu.VMEM((local, rows, ff), F32),
            pltpu.VMEM((RING, 2, WIDTH, ff), BF16),
            pltpu.VMEM((2, 2, chips, tokens, WIDTH), BF16),
            pltpu.VMEM((local, rows, WIDTH), BF16),
            pltpu.VMEM((n, local * slots, tokens), BF16),
            pltpu.VMEM((n, local * slots, tokens), BF16),
            pltpu.VMEM((n, *mt.shape), BF16),
            pltpu.VMEM((2, rows, ff), BF16),
            dma((n,)), dma((n,)), dma((3,)), dma((2,)), dma((3,)),
            dma((chunks,)), dma((chunks,)), dma((chunks,)), dma((chunks,)), dma((chunks,)),
            dma((RING,)), dma((chunks,)), dma((2,)), dma((4,)),
        ],
        compiler_params=pltpu.CompilerParams(
            collective_id=0, has_side_effects=True, vmem_limit_bytes=62 * 2**20
        ),
        cost_estimate=pl.CostEstimate(flops=flops, bytes_accessed=moved, transcendentals=0),
    )(x, mt, wg, wu, sg, su)


def down_kernel(n, local, slots, h, hs, gt, wd, sd, y, hv, hsv, gm, wbuf, outs, part, sh, pair_s, pair_r, hop_s, hop_r,
                end_s, end_r, ys, insem, wsem, pair_ss, pair_rs, hop_ss, hop_rs, end_ss, end_rs, ysem):
    me, chips, chip, core, right, left, across = places(n)
    dev_r, dev_l, dev_p = right * 2 + core, left * 2 + core, chip * 2 + 1 - core
    tokens, ff = hs.shape
    chunks = wd.shape[2] // WIDTH
    half = tokens // 2
    per = local + 1
    steps = chunks * per

    def cols(c):
        return pl.ds(pl.multiple_of(c * WIDTH, WIDTH), WIDTH)

    def fetch(t):
        slot = lax.rem(t, RING)
        c, e = lax.div(t, per), lax.rem(t, per)

        @pl.when(e < local)
        def _():
            pltpu.make_async_copy(wd.at[e, :, cols(c)], wbuf.at[slot], wsem.at[slot]).start()

        @pl.when(e == local)
        def _():
            pltpu.make_async_copy(sd.at[:, cols(c)], wbuf.at[slot], wsem.at[slot]).start()

    fetch(jnp.int32(0))
    for e in range(local):
        pltpu.make_async_copy(h.at[e], hv.at[e], insem.at[e]).start()
    fetch(jnp.int32(1))
    pltpu.make_async_copy(hs, hsv, insem.at[local]).start()
    pltpu.make_async_copy(gt, gm, insem.at[local + 1]).start()

    barrier = pltpu.get_barrier_semaphore()
    for dev in (dev_r, dev_l, dev_p):
        pl.semaphore_signal(barrier, inc=1, device_id={"ep": dev}, device_id_type=MESH)
    pl.semaphore_wait(barrier, 3)

    def first_hop(c):
        k, b = lax.rem(c, 3), lax.rem(c, 2)

        @pl.when(c >= 2)
        def _():
            for i in range(2):
                wait(hop_s.at[b, i], hop_ss.at[b, i])

        wait(pair_r.at[c], pair_rs.at[c])
        v = (part[k, across] + pair_r[c, across].astype(F32)).astype(BF16)
        hop_s[b, 0] = v[:half]
        hop_s[b, 1] = v[half:]
        send(hop_s.at[b, 0], hop_r.at[c, 0], hop_ss.at[b, 0], hop_rs.at[c, 0], dev_r)
        send(hop_s.at[b, 1], hop_r.at[c, 1], hop_ss.at[b, 1], hop_rs.at[c, 1], dev_l)

    def second_hop(c):
        k, b = lax.rem(c, 3), lax.rem(c, 2)

        @pl.when(c >= 2)
        def _():
            for i in range(2):
                wait(end_s.at[b, i], end_ss.at[b, i])

        up, lo = pl.ds(0, half), pl.ds(half, half)
        for i, to in ((0, right), (1, left)):
            wait(hop_r.at[c, i], hop_rs.at[c, i])
            rows, others = (up, lo) if i == 0 else (lo, up)
            v = part[k, to, rows] + pair_r[c, to, rows].astype(F32) + hop_r[c, i].astype(F32)
            end_s[b, i, rows] = v.astype(BF16)
            v = part[k, to, others] + pair_r[c, to, others].astype(F32)
            end_s[b, i, others] = v.astype(BF16)
            send(end_s.at[b, i], end_r.at[c, i], end_ss.at[b, i], end_rs.at[c, i], (dev_r, dev_l)[i])

    def finish(c):
        k, b = lax.rem(c, 3), lax.rem(c, 2)

        @pl.when(c >= 2)
        def _():
            wait(ys.at[b], ysem.at[b])

        for i in range(2):
            wait(end_r.at[c, i], end_rs.at[c, i])
        v = part[k, chip] + pair_r[c, chip].astype(F32) + end_r[c, 0].astype(F32) + end_r[c, 1].astype(F32)
        ys[b] = (v + sh[k]).astype(BF16)
        pltpu.make_async_copy(ys.at[b], y.at[:, cols(c)], ysem.at[b]).start()

    @pl.loop(0, steps)
    def _(t):
        c, e = lax.div(t, per), lax.rem(t, per)
        slot = lax.rem(t, RING)

        @pl.when((e == 1) & (c >= 1))
        def _():
            first_hop(c - 1)

        @pl.when((e == 2) & (c >= 2))
        def _():
            second_hop(c - 2)

        @pl.when((e == 4) & (c >= 3))
        def _():
            finish(c - 3)

        @pl.when((c == 0) & (e < local))
        def _():
            wait(hv.at[e], insem.at[e])

        @pl.when(t == local)
        def _():
            wait(hs, insem.at[local])
            wait(gt, insem.at[local + 1])

        wait(wbuf.at[slot], wsem.at[slot])

        @pl.when(t + 2 < steps)
        def _():
            fetch(t + 2)

        @pl.when(e < local)
        def _():
            v = mm(hv[e], wbuf[slot]).astype(BF16)
            for q in range(n):
                outs[q, pl.ds(pl.multiple_of(e * slots, slots), slots)] = v[q * slots : (q + 1) * slots]

        @pl.when(e == local)
        def _():
            b, k = lax.rem(c, 2), lax.rem(c, 3)

            @pl.when(c >= 2)
            def _():
                wait(pair_s.at[b], pair_ss.at[b])

            def combined(q):
                return lax.dot_general(gm[q], outs[q], (((0,), (0,)), ((), ())), preferred_element_type=F32)

            for i in range(chips):
                pair_s[b, i] = combined((1 - core) * chips + i).astype(BF16)
            send(pair_s.at[b], pair_r.at[c], pair_ss.at[b], pair_rs.at[c], dev_p)
            for i in range(chips):
                part[k, i] = combined(core * chips + i)
            sh[k] = mm(hsv[...], wbuf[slot])

    end = chunks - 1
    second_hop(jnp.int32(end - 1))
    first_hop(jnp.int32(end))
    finish(jnp.int32(end - 2))
    second_hop(jnp.int32(end))
    finish(jnp.int32(end - 1))
    finish(jnp.int32(end))
    for b in range(2):
        wait(pair_s.at[b], pair_ss.at[b])
        wait(ys.at[b], ysem.at[b])
        for i in range(2):
            wait(hop_s.at[b, i], hop_ss.at[b, i])
            wait(end_s.at[b, i], end_ss.at[b, i])


def down(n, slots, h, hs, gt, wd, sd):
    local, rows, ff = h.shape
    tokens, d = hs.shape[0], wd.shape[2]
    chunks, chips, half = d // WIDTH, n // 2, tokens // 2
    dma = pltpu.SemaphoreType.DMA
    flops = 2 * (rows * local + tokens) * d * ff
    return pl.pallas_call(
        functools.partial(down_kernel, n, local, slots),
        out_shape=jax.ShapeDtypeStruct((tokens, d), BF16),
        in_specs=[ANY] * 5,
        out_specs=ANY,
        scratch_shapes=[
            pltpu.VMEM(h.shape, BF16),
            pltpu.VMEM(hs.shape, BF16),
            pltpu.VMEM(gt.shape, BF16),
            pltpu.VMEM((RING, ff, WIDTH), BF16),
            pltpu.VMEM((n, local * slots, WIDTH), BF16),
            pltpu.VMEM((3, chips, tokens, WIDTH), F32),
            pltpu.VMEM((3, tokens, WIDTH), F32),
            pltpu.VMEM((2, chips, tokens, WIDTH), BF16),
            pltpu.VMEM((chunks, chips, tokens, WIDTH), BF16),
            pltpu.VMEM((2, 2, half, WIDTH), BF16),
            pltpu.VMEM((chunks, 2, half, WIDTH), BF16),
            pltpu.VMEM((2, 2, tokens, WIDTH), BF16),
            pltpu.VMEM((chunks, 2, tokens, WIDTH), BF16),
            pltpu.VMEM((2, tokens, WIDTH), BF16),
            dma((local + 2,)), dma((RING,)), dma((2,)), dma((chunks,)), dma((2, 2)), dma((chunks, 2)),
            dma((2, 2)), dma((chunks, 2)), dma((2,)),
        ],
        compiler_params=pltpu.CompilerParams(
            collective_id=1, has_side_effects=True, vmem_limit_bytes=62 * 2**20
        ),
        cost_estimate=pl.CostEstimate(flops=flops, bytes_accessed=2 * (local + 1) * d * ff, transcendentals=0),
    )(h, hs, gt, wd, sd)


def solution(mesh):
    n = mesh.shape["ep"]

    def body(x, expert, slot, gate, w_gate, w_up, w_down, s_gate, s_up, s_down):
        x, expert, slot, gate = x[0, 0], expert[0, 0], slot[0, 0], gate[0, 0]
        (tokens, top), local = expert.shape, w_gate.shape[0]
        slots = 5 * tokens * top // (4 * local * n)
        parts = [expert.astype(BF16), jnp.minimum(slot, slots).astype(BF16), gate.astype(BF16)]
        mt = jnp.concatenate([p.T for p in parts] + [jnp.zeros((top, tokens), BF16)])
        h, hs, gt, _ = up(n, slots, x, mt, w_gate, w_up, s_gate, s_up)
        return down(n, slots, h, hs, gt, w_down, s_down)[None, None]

    a, e, r = P("dp", "ep", None, None), P("ep", None, None), P(None, None)
    return jax.shard_map(body, mesh=mesh, in_specs=(a, a, a, a, e, e, e, r, r, r), out_specs=a, check_vma=False)
```

```python
import functools

import jax
import jax.numpy as jnp
from jax import lax
from jax.experimental import pallas as pl
from jax.experimental.pallas import tpu as pltpu
from jax.sharding import PartitionSpec as P

F32, BF16 = jnp.float32, jnp.bfloat16
MESH = pl.DeviceIdType.MESH
ANY = pl.BlockSpec(memory_space=pl.ANY)
VM = pl.BlockSpec(memory_space=pltpu.VMEM)
WIDTH = 512
TILE = 256
DOWN = 512
RING = 3


def mm(a, b):
    return jnp.dot(a, b, preferred_element_type=F32)


def silu(v):
    return v * (1.0 / (1.0 + jnp.exp(-v)))


def places(n):
    me = lax.axis_index("ep")
    chips = n // 2
    chip, core = lax.div(me, 2), lax.rem(me, 2)
    right, left = lax.rem(chip + 1, chips), lax.rem(chip + chips - 1, chips)
    across = lax.rem(chip + 2, chips)
    return me, chips, chip, core, right, left, across


def send(src, dst, send_sem, recv_sem, device):
    pltpu.make_async_remote_copy(
        src_ref=src, dst_ref=dst, send_sem=send_sem, recv_sem=recv_sem, device_id={"ep": device}, device_id_type=MESH
    ).start()


def wait(ref, sem):
    pltpu.make_async_copy(ref, ref, sem).wait()


def up_kernel(n, local, slots, x, mt, wg, wu, sg, su, h, hs, gt, xg, acc_g, acc_u, wbuf, xv, z, dm, gm, meta, hst,
              meta_send, meta_recv, own_send, fwd_send, pass_send, recv_l, recv_r, recv_a, recv_b, recv_p,
              wsem, xsem, ldsem, osem):
    me, chips, chip, core, right, left, across = places(n)
    dev_r, dev_l, dev_p = right * 2 + core, left * 2 + core, chip * 2 + 1 - core
    tokens, d = x.shape
    ff = sg.shape[1]
    chunks = d // WIDTH
    half = tokens // 2
    rows = n * slots
    top = mt.shape[0] // 4

    def cols(c):
        return pl.ds(pl.multiple_of(c * WIDTH, WIDTH), WIDTH)

    def fetch_shared(c):
        slot = c % local
        pltpu.make_async_copy(sg.at[cols(c), :], wbuf.at[slot, 0], wsem.at[slot]).start()
        pltpu.make_async_copy(su.at[cols(c), :], wbuf.at[slot, 1], wsem.at[slot]).start()

    def fetch_at(c, e):
        pltpu.make_async_copy(wg.at[e, cols(c), :], wbuf.at[e, 0], wsem.at[e]).start()
        pltpu.make_async_copy(wu.at[e, cols(c), :], wbuf.at[e, 1], wsem.at[e]).start()

    for i in range(local):
        fetch_shared(i)

    def piece(c):
        return xv.at[c // 8, (c % 8) // 4, c % 4]

    for c in range(chunks):
        pltpu.make_async_copy(x.at[:, cols(c)], piece(c), xsem.at[c]).start()

    barrier = pltpu.get_barrier_semaphore()
    for r in range(1, n):
        pl.semaphore_signal(barrier, inc=1, device_id={"ep": lax.rem(me + r, n)}, device_id_type=MESH)
    pl.semaphore_wait(barrier, n - 1)

    mine = core * chips + chip

    def own(c, i):
        part = pl.ds(i * half, half)
        src, dst = x.at[part, cols(c)], xg.at[c, core, chip, part]
        send(src, dst, own_send.at[0], recv_l.at[c], dev_r)
        send(src, dst, own_send.at[1], recv_r.at[c], dev_l)
        send(src, dst, own_send.at[2], recv_p.at[c], dev_p)

    def forward(c):
        piece_l, piece_r = xg.at[c, core, left], xg.at[c, core, right]
        wait(piece_l, recv_l.at[c])
        upper = piece_l.at[pl.ds(0, half)]
        send(upper, upper, fwd_send.at[0], recv_a.at[c], dev_r)
        wait(piece_r, recv_r.at[c])
        lower = piece_r.at[pl.ds(half, half)]
        send(lower, lower, fwd_send.at[1], recv_b.at[c], dev_l)
        send(piece_l, piece_l, pass_send.at[0], recv_p.at[c], dev_p)
        send(piece_r, piece_r, pass_send.at[1], recv_p.at[c], dev_p)

    def last_hop(c):
        piece_o = xg.at[c, core, across]
        wait(piece_o.at[pl.ds(0, half)], recv_a.at[c])
        wait(piece_o.at[pl.ds(half, half)], recv_b.at[c])
        send(piece_o, piece_o, pass_send.at[2], recv_p.at[c], dev_p)

    def load(c):
        slot = lax.rem(c, 2)
        wait(xg.at[c, 1 - core], recv_p.at[c])
        pltpu.make_async_copy(xg.at[c, 1 - core], xv.at[slot, 1 - core], ldsem.at[slot]).start()
        pltpu.make_async_copy(x.at[:, cols(c)], xv.at[slot, core, chip], ldsem.at[slot]).start()
        for other in (left, right, across):
            pltpu.make_async_copy(xg.at[c, core, other], xv.at[slot, core, other], ldsem.at[slot]).start()

    own(0, 0)
    own(0, 1)
    for r in range(1, n):
        send(mt, meta.at[mine], meta_send.at[r], meta_recv.at[mine], lax.rem(me + r, n))
    meta[mine] = mt[...]

    tiles = [(i, min(i + TILE, ff)) for i in range(0, ff, TILE)]

    def shared_step(c):
        slot = c % local
        wait(wbuf.at[slot], wsem.at[slot])
        if c >= 1 and c + local - 1 < chunks:
            fetch_shared(c + local - 1)
        elif c >= 1 and c + local - 1 - chunks < local - 2:
            fetch_at(0, c + local - 1 - chunks)
        wait(piece(c), xsem.at[c])
        xc = piece(c)[...]
        for lo, hi in tiles:
            for k, acc in ((0, acc_g), (1, acc_u)):
                v = mm(xc, wbuf[slot, k, :, lo:hi])
                acc[0, :tokens, lo:hi] = v if c == 0 else acc[0, :tokens, lo:hi] + v

    for c in range(chunks):
        if c == chunks - 2:
            forward(0)
            own(1, 0)
            own(1, 1)
            own(2, 0)
        shared_step(c)
    hst[0, :tokens] = (silu(acc_g[0, :tokens]) * acc_u[0, :tokens]).astype(BF16)
    pltpu.make_async_copy(hst.at[0, pl.ds(0, tokens)], hs, osem.at[0]).start()

    for r in range(1, n):
        src = lax.rem(me + r, n)
        q = lax.rem(src, 2) * chips + lax.div(src, 2)
        wait(meta.at[q], meta_recv.at[q])
    first = (me * local).astype(F32)

    @pl.loop(0, n)
    def _(q):
        m = meta[q].astype(F32)
        e, s, g = m[0:top], m[top : 2 * top], m[2 * top : 3 * top]
        ok = (e >= first) & (e < first + local) & (s < slots)
        key = jnp.where(ok, (e - first) * slots + s, -1.0)
        for i in range(local):
            row = lax.broadcasted_iota(jnp.int32, (slots, tokens), 0).astype(F32) + float(i * slots)
            hot = jnp.zeros((slots, tokens), F32)
            weight = jnp.zeros((slots, tokens), F32)
            for k in range(top):
                hit = row == key[k : k + 1]
                hot = jnp.where(hit, 1.0, hot)
                weight = jnp.where(hit, g[k : k + 1], weight)
            dm[q, i * slots : (i + 1) * slots] = hot.astype(BF16)
            gm[q, i * slots : (i + 1) * slots] = weight.astype(BF16)

    last_hop(0)
    pltpu.make_async_copy(gm, gt, osem.at[1]).start()
    wait(hs, osem.at[0])
    load(0)

    def dispatch(c):
        slot = lax.rem(c, 2)
        wait(xv.at[slot], ldsem.at[slot])
        for q in range(n):
            v = mm(dm[q], xv[slot, q // chips, q % chips]).astype(BF16)
            for i in range(local):
                z[i, q * slots : (q + 1) * slots] = v[i * slots : (i + 1) * slots]

    @pl.loop(0, chunks - 1)
    def _(c):
        forward(c + 1)

        @pl.when(c + 2 < chunks)
        def _():
            own(c + 2, 1)

        @pl.when(c + 3 < chunks)
        def _():
            own(c + 3, 0)

        start, groups = 0, (local - 2, 1, 1)
        for i, size in enumerate(groups):
            group = range(start, start + size)
            start += size
            if i == 1:
                last_hop(c + 1)
            if i == 2:
                load(c + 1)
            for e in group:
                wait(wbuf.at[e], wsem.at[e])
            if i == 0:
                for e in range(local - 2, local):
                    fetch_at(c, e)
                dispatch(c)
            if i == 1:
                for e in range(local - 2):
                    fetch_at(c + 1, e)
            for e in group:
                for lo, hi in tiles:
                    for k, acc in ((0, acc_g), (1, acc_u)):
                        v = mm(z[e], wbuf[e, k, :, lo:hi])
                        acc[e, :, lo:hi] = jnp.where(c == 0, 0.0, acc[e, :, lo:hi]) + v

    for e in range(local - 2, local):
        fetch_at(chunks - 1, e)
    dispatch(jnp.int32(chunks - 1))

    for e in range(local):
        slot, to = e, e % 2
        wait(wbuf.at[slot], wsem.at[slot])
        if e >= 2:
            wait(hst.at[to], osem.at[2 + to])
        for lo, hi in tiles:
            g = acc_g[e, :, lo:hi] + mm(z[e], wbuf[slot, 0, :, lo:hi])
            u = acc_u[e, :, lo:hi] + mm(z[e], wbuf[slot, 1, :, lo:hi])
            hst[to, :, lo:hi] = (silu(g) * u).astype(BF16)
        pltpu.make_async_copy(hst.at[to], h.at[e], osem.at[2 + to]).start()

    for to in range(2):
        wait(hst.at[to], osem.at[2 + to])
    wait(gm, osem.at[1])
    for i in range(3):
        wait(x, own_send.at[i])
        wait(x, pass_send.at[i])
    for i in range(2):
        wait(x.at[pl.ds(0, half)], fwd_send.at[i])
    for r in range(1, n):
        wait(mt, meta_send.at[r])


def up(n, slots, x, mt, wg, wu, sg, su):
    tokens, d = x.shape
    local, _, ff = wg.shape
    chunks, rows, chips = d // WIDTH, n * slots, n // 2
    dma = pltpu.SemaphoreType.DMA
    flops = 2 * (rows * local + tokens) * d * ff * 2
    moved = 2 * (2 * local + 2) * d * ff
    return pl.pallas_call(
        functools.partial(up_kernel, n, local, slots),
        out_shape=[
            jax.ShapeDtypeStruct((local, rows, ff), BF16),
            jax.ShapeDtypeStruct((tokens, ff), BF16),
            jax.ShapeDtypeStruct((n, local * slots, tokens), BF16),
            jax.ShapeDtypeStruct((chunks, 2, chips, tokens, WIDTH), BF16),
        ],
        in_specs=[ANY, VM, ANY, ANY, ANY, ANY],
        out_specs=[ANY] * 4,
        scratch_shapes=[
            pltpu.VMEM((local, rows, ff), F32),
            pltpu.VMEM((local, rows, ff), F32),
            pltpu.VMEM((local, 2, WIDTH, ff), BF16),
            pltpu.VMEM((2, 2, chips, tokens, WIDTH), BF16),
            pltpu.VMEM((local, rows, WIDTH), BF16),
            pltpu.VMEM((n, local * slots, tokens), BF16),
            pltpu.VMEM((n, local * slots, tokens), BF16),
            pltpu.VMEM((n, *mt.shape), BF16),
            pltpu.VMEM((2, rows, ff), BF16),
            dma((n,)), dma((n,)), dma((3,)), dma((2,)), dma((3,)),
            dma((chunks,)), dma((chunks,)), dma((chunks,)), dma((chunks,)), dma((chunks,)),
            dma((local,)), dma((chunks,)), dma((2,)), dma((4,)),
        ],
        compiler_params=pltpu.CompilerParams(
            collective_id=0, has_side_effects=True, vmem_limit_bytes=66 * 10**6
        ),
        cost_estimate=pl.CostEstimate(flops=flops, bytes_accessed=moved, transcendentals=0),
    )(x, mt, wg, wu, sg, su)


def down_kernel(n, local, slots, h, hs, gt, wd, sd, y, hv, hsv, gm, wbuf, outs, part, sh, pair_s, pair_r, hop_s, hop_r,
                end_s, end_r, ys, insem, wsem, pair_ss, pair_rs, hop_ss, hop_rs, end_ss, end_rs, ysem):
    me, chips, chip, core, right, left, across = places(n)
    dev_r, dev_l, dev_p = right * 2 + core, left * 2 + core, chip * 2 + 1 - core
    tokens, ff = hs.shape
    chunks = wd.shape[2] // DOWN
    half = tokens // 2
    per = local + 1
    steps = chunks * per

    def cols(c):
        return pl.ds(pl.multiple_of(c * DOWN, DOWN), DOWN)

    def fetch(t):
        slot = lax.rem(t, RING)
        c, e = lax.div(t, per), lax.rem(t, per)

        @pl.when(e < local)
        def _():
            pltpu.make_async_copy(wd.at[e, :, cols(c)], wbuf.at[slot], wsem.at[slot]).start()

        @pl.when(e == local)
        def _():
            pltpu.make_async_copy(sd.at[:, cols(c)], wbuf.at[slot], wsem.at[slot]).start()

    fetch(jnp.int32(0))
    for e in range(local):
        pltpu.make_async_copy(h.at[e], hv.at[e], insem.at[e]).start()
    fetch(jnp.int32(1))
    pltpu.make_async_copy(hs, hsv, insem.at[local]).start()
    pltpu.make_async_copy(gt, gm, insem.at[local + 1]).start()

    barrier = pltpu.get_barrier_semaphore()
    for dev in (dev_r, dev_l, dev_p):
        pl.semaphore_signal(barrier, inc=1, device_id={"ep": dev}, device_id_type=MESH)
    pl.semaphore_wait(barrier, 3)

    def first_hop(c):
        k, b = lax.rem(c, 3), lax.rem(c, 2)

        @pl.when(c >= 2)
        def _():
            for i in range(2):
                wait(hop_s.at[b, i], hop_ss.at[b, i])

        wait(pair_r.at[c], pair_rs.at[c])
        v = (part[k, across] + pair_r[c, across].astype(F32)).astype(BF16)
        hop_s[b, 0] = v[:half]
        hop_s[b, 1] = v[half:]
        send(hop_s.at[b, 0], hop_r.at[c, 0], hop_ss.at[b, 0], hop_rs.at[c, 0], dev_r)
        send(hop_s.at[b, 1], hop_r.at[c, 1], hop_ss.at[b, 1], hop_rs.at[c, 1], dev_l)

    def second_hop(c):
        k, b = lax.rem(c, 3), lax.rem(c, 2)

        @pl.when(c >= 2)
        def _():
            for i in range(2):
                wait(end_s.at[b, i], end_ss.at[b, i])

        up, lo = pl.ds(0, half), pl.ds(half, half)
        for i, to in ((0, right), (1, left)):
            wait(hop_r.at[c, i], hop_rs.at[c, i])
            rows, others = (up, lo) if i == 0 else (lo, up)
            v = part[k, to, rows] + pair_r[c, to, rows].astype(F32) + hop_r[c, i].astype(F32)
            end_s[b, i, rows] = v.astype(BF16)
            v = part[k, to, others] + pair_r[c, to, others].astype(F32)
            end_s[b, i, others] = v.astype(BF16)
            send(end_s.at[b, i], end_r.at[c, i], end_ss.at[b, i], end_rs.at[c, i], (dev_r, dev_l)[i])

    def finish(c):
        k, b = lax.rem(c, 3), lax.rem(c, 2)

        @pl.when(c >= 2)
        def _():
            wait(ys.at[b], ysem.at[b])

        for i in range(2):
            wait(end_r.at[c, i], end_rs.at[c, i])
        v = part[k, chip] + pair_r[c, chip].astype(F32) + end_r[c, 0].astype(F32) + end_r[c, 1].astype(F32)
        ys[b] = (v + sh[k]).astype(BF16)
        pltpu.make_async_copy(ys.at[b], y.at[:, cols(c)], ysem.at[b]).start()

    @pl.loop(0, steps)
    def _(t):
        c, e = lax.div(t, per), lax.rem(t, per)
        slot = lax.rem(t, RING)

        @pl.when((e == 1) & (c >= 1))
        def _():
            first_hop(c - 1)

        @pl.when((e == 2) & (c >= 2))
        def _():
            second_hop(c - 2)

        @pl.when((e == 4) & (c >= 3))
        def _():
            finish(c - 3)

        @pl.when((c == 0) & (e < local))
        def _():
            wait(hv.at[e], insem.at[e])

        @pl.when(t == local)
        def _():
            wait(hs, insem.at[local])
            wait(gt, insem.at[local + 1])

        wait(wbuf.at[slot], wsem.at[slot])

        @pl.when(t + 2 < steps)
        def _():
            fetch(t + 2)

        @pl.when(e < local)
        def _():
            v = mm(hv[e], wbuf[slot]).astype(BF16)
            for q in range(n):
                outs[q, pl.ds(pl.multiple_of(e * slots, slots), slots)] = v[q * slots : (q + 1) * slots]

        @pl.when(e == local)
        def _():
            b, k = lax.rem(c, 2), lax.rem(c, 3)

            @pl.when(c >= 2)
            def _():
                wait(pair_s.at[b], pair_ss.at[b])

            def combined(q):
                return lax.dot_general(gm[q], outs[q], (((0,), (0,)), ((), ())), preferred_element_type=F32)

            for i in range(chips):
                pair_s[b, i] = combined((1 - core) * chips + i).astype(BF16)
            send(pair_s.at[b], pair_r.at[c], pair_ss.at[b], pair_rs.at[c], dev_p)
            for i in range(chips):
                part[k, i] = combined(core * chips + i)
            sh[k] = mm(hsv[...], wbuf[slot])

    end = chunks - 1
    second_hop(jnp.int32(end - 1))
    first_hop(jnp.int32(end))
    finish(jnp.int32(end - 2))
    second_hop(jnp.int32(end))
    finish(jnp.int32(end - 1))
    finish(jnp.int32(end))
    for b in range(2):
        wait(pair_s.at[b], pair_ss.at[b])
        wait(ys.at[b], ysem.at[b])
        for i in range(2):
            wait(hop_s.at[b, i], hop_ss.at[b, i])
            wait(end_s.at[b, i], end_ss.at[b, i])


def down(n, slots, h, hs, gt, wd, sd):
    local, rows, ff = h.shape
    tokens, d = hs.shape[0], wd.shape[2]
    chunks, chips, half = d // DOWN, n // 2, tokens // 2
    dma = pltpu.SemaphoreType.DMA
    flops = 2 * (rows * local + tokens) * d * ff
    return pl.pallas_call(
        functools.partial(down_kernel, n, local, slots),
        out_shape=jax.ShapeDtypeStruct((tokens, d), BF16),
        in_specs=[ANY] * 5,
        out_specs=ANY,
        scratch_shapes=[
            pltpu.VMEM(h.shape, BF16),
            pltpu.VMEM(hs.shape, BF16),
            pltpu.VMEM(gt.shape, BF16),
            pltpu.VMEM((RING, ff, DOWN), BF16),
            pltpu.VMEM((n, local * slots, DOWN), BF16),
            pltpu.VMEM((3, chips, tokens, DOWN), F32),
            pltpu.VMEM((3, tokens, DOWN), F32),
            pltpu.VMEM((2, chips, tokens, DOWN), BF16),
            pltpu.VMEM((chunks, chips, tokens, DOWN), BF16),
            pltpu.VMEM((2, 2, half, DOWN), BF16),
            pltpu.VMEM((chunks, 2, half, DOWN), BF16),
            pltpu.VMEM((2, 2, tokens, DOWN), BF16),
            pltpu.VMEM((chunks, 2, tokens, DOWN), BF16),
            pltpu.VMEM((2, tokens, DOWN), BF16),
            dma((local + 2,)), dma((RING,)), dma((2,)), dma((chunks,)), dma((2, 2)), dma((chunks, 2)),
            dma((2, 2)), dma((chunks, 2)), dma((2,)),
        ],
        compiler_params=pltpu.CompilerParams(
            collective_id=1, has_side_effects=True, vmem_limit_bytes=62 * 2**20
        ),
        cost_estimate=pl.CostEstimate(flops=flops, bytes_accessed=2 * (local + 1) * d * ff, transcendentals=0),
    )(h, hs, gt, wd, sd)


def solution(mesh):
    n = mesh.shape["ep"]

    def body(x, expert, slot, gate, w_gate, w_up, w_down, s_gate, s_up, s_down):
        x, expert, slot, gate = x[0, 0], expert[0, 0], slot[0, 0], gate[0, 0]
        (tokens, top), local = expert.shape, w_gate.shape[0]
        slots = 5 * tokens * top // (4 * local * n)
        parts = [expert.astype(BF16), jnp.minimum(slot, slots).astype(BF16), gate.astype(BF16)]
        mt = jnp.concatenate([p.T for p in parts] + [jnp.zeros((top, tokens), BF16)])
        h, hs, gt, _ = up(n, slots, x, mt, w_gate, w_up, s_gate, s_up)
        return down(n, slots, h, hs, gt, w_down, s_down)[None, None]

    a, e, r = P("dp", "ep", None, None), P("ep", None, None), P(None, None)
    return jax.shard_map(body, mesh=mesh, in_specs=(a, a, a, a, e, e, e, r, r, r), out_specs=a, check_vma=False)
```

```python
import functools

import jax
import jax.numpy as jnp
from jax import lax
from jax.experimental import pallas as pl
from jax.experimental.pallas import tpu as pltpu
from jax.sharding import PartitionSpec as P

F32, BF16 = jnp.float32, jnp.bfloat16
MESH = pl.DeviceIdType.MESH
ANY = pl.BlockSpec(memory_space=pl.ANY)
VM = pl.BlockSpec(memory_space=pltpu.VMEM)
WIDTH = 512
TILE = 256
DOWN = 512
RING = 3


def mm(a, b):
    return jnp.dot(a, b, preferred_element_type=F32)


def silu(v):
    return v * (1.0 / (1.0 + jnp.exp(-v)))


def places(n):
    me = lax.axis_index("ep")
    chips = n // 2
    chip, core = lax.div(me, 2), lax.rem(me, 2)
    right, left = lax.rem(chip + 1, chips), lax.rem(chip + chips - 1, chips)
    across = lax.rem(chip + 2, chips)
    return me, chips, chip, core, right, left, across


def send(src, dst, send_sem, recv_sem, device):
    pltpu.make_async_remote_copy(
        src_ref=src, dst_ref=dst, send_sem=send_sem, recv_sem=recv_sem, device_id={"ep": device}, device_id_type=MESH
    ).start()


def wait(ref, sem):
    pltpu.make_async_copy(ref, ref, sem).wait()


def up_kernel(n, local, slots, x, expert, slot_in, gate, wg, wu, sg, su, h, hs, gt, xg, acc_g, acc_u, wbuf, xv, z, dm, gm, meta, hst,
              meta_send, meta_recv, own_send, fwd_send, pass_send, recv_l, recv_r, recv_a, recv_b, recv_p,
              wsem, xsem, ldsem, osem):
    me, chips, chip, core, right, left, across = places(n)
    dev_r, dev_l, dev_p = right * 2 + core, left * 2 + core, chip * 2 + 1 - core
    tokens, d = x.shape
    ff = sg.shape[1]
    chunks = d // WIDTH
    half = tokens // 2
    rows = n * slots
    top = expert.shape[0]

    def cols(c):
        return pl.ds(pl.multiple_of(c * WIDTH, WIDTH), WIDTH)

    def fetch_shared(c):
        slot = c % local
        pltpu.make_async_copy(sg.at[cols(c), :], wbuf.at[slot, 0], wsem.at[slot]).start()
        pltpu.make_async_copy(su.at[cols(c), :], wbuf.at[slot, 1], wsem.at[slot]).start()

    def fetch_at(c, e):
        pltpu.make_async_copy(wg.at[e, cols(c), :], wbuf.at[e, 0], wsem.at[e]).start()
        pltpu.make_async_copy(wu.at[e, cols(c), :], wbuf.at[e, 1], wsem.at[e]).start()

    for i in range(local):
        fetch_shared(i)

    def piece(c):
        return xv.at[c // 8, (c % 8) // 4, c % 4]

    for c in range(chunks):
        pltpu.make_async_copy(x.at[:, cols(c)], piece(c), xsem.at[c]).start()

    mine = core * chips + chip
    known = [expert[...].astype(F32), jnp.minimum(slot_in[...], slots).astype(F32), gate[...]]
    known.append(jnp.zeros((top, tokens), F32))
    meta[mine] = jnp.concatenate(known).astype(BF16)

    barrier = pltpu.get_barrier_semaphore()
    for r in range(1, n):
        pl.semaphore_signal(barrier, inc=1, device_id={"ep": lax.rem(me + r, n)}, device_id_type=MESH)
    pl.semaphore_wait(barrier, n - 1)

    upper, lower = pl.ds(0, half), pl.ds(half, half)

    def own(c):
        src, dst = x.at[:, cols(c)], xg.at[c, core, chip]
        for i, (to_r, to_l) in enumerate(((upper, lower), (lower, upper))):
            send(src.at[to_r], dst.at[to_r], own_send.at[0], recv_l.at[c, i], dev_r)
            send(src.at[to_l], dst.at[to_l], own_send.at[1], recv_r.at[c, i], dev_l)
        send(src, dst, own_send.at[2], recv_p.at[c], dev_p)

    def forward(c):
        from_l, from_r = xg.at[c, core, left, upper], xg.at[c, core, right, lower]
        wait(from_l, recv_l.at[c, 0])
        send(from_l, from_l, fwd_send.at[0], recv_a.at[c], dev_r)
        wait(from_r, recv_r.at[c, 0])
        send(from_r, from_r, fwd_send.at[1], recv_b.at[c], dev_l)

    def hand_over(c):
        piece_l, piece_r = xg.at[c, core, left], xg.at[c, core, right]
        wait(piece_l.at[lower], recv_l.at[c, 1])
        send(piece_l, piece_l, pass_send.at[0], recv_p.at[c], dev_p)
        wait(piece_r.at[upper], recv_r.at[c, 1])
        send(piece_r, piece_r, pass_send.at[1], recv_p.at[c], dev_p)

    def last_hop(c):
        piece_o = xg.at[c, core, across]
        wait(piece_o.at[pl.ds(0, half)], recv_a.at[c])
        wait(piece_o.at[pl.ds(half, half)], recv_b.at[c])
        send(piece_o, piece_o, pass_send.at[2], recv_p.at[c], dev_p)

    def load(c):
        slot = lax.rem(c, 2)
        wait(xg.at[c, 1 - core], recv_p.at[c])
        pltpu.make_async_copy(xg.at[c, 1 - core], xv.at[slot, 1 - core], ldsem.at[slot]).start()
        pltpu.make_async_copy(x.at[:, cols(c)], xv.at[slot, core, chip], ldsem.at[slot]).start()
        for other in (left, right, across):
            pltpu.make_async_copy(xg.at[c, core, other], xv.at[slot, core, other], ldsem.at[slot]).start()

    own(0)
    for r in range(1, n):
        send(meta.at[mine], meta.at[mine], meta_send.at[r], meta_recv.at[mine], lax.rem(me + r, n))

    tiles = [(i, min(i + TILE, ff)) for i in range(0, ff, TILE)]

    def shared_step(c):
        slot = c % local
        wait(wbuf.at[slot], wsem.at[slot])
        if c >= 1 and c + local - 1 < chunks:
            fetch_shared(c + local - 1)
        elif c >= 1 and c + local - 1 - chunks < local - 2:
            fetch_at(0, c + local - 1 - chunks)
        wait(piece(c), xsem.at[c])
        xc = piece(c)[...]
        for lo, hi in tiles:
            for k, acc in ((0, acc_g), (1, acc_u)):
                v = mm(xc, wbuf[slot, k, :, lo:hi])
                acc[0, :tokens, lo:hi] = v if c == 0 else acc[0, :tokens, lo:hi] + v

    def build():
        for r in range(1, n):
            src = lax.rem(me + r, n)
            q = lax.rem(src, 2) * chips + lax.div(src, 2)
            wait(meta.at[q], meta_recv.at[q])
        first = (me * local).astype(F32)

        @pl.loop(0, n)
        def _(q):
            m = meta[q].astype(F32)
            e, s, g = m[0:top], m[top : 2 * top], m[2 * top : 3 * top]
            row = lax.broadcasted_iota(jnp.int32, (slots, tokens), 0).astype(F32)
            for i in range(local):
                chosen = e == first + float(i)
                place = jnp.max(jnp.where(chosen, s, -1.0), axis=0, keepdims=True)
                share = jnp.sum(jnp.where(chosen, g, 0.0), axis=0, keepdims=True)
                hit = row == place
                hot = jnp.where(hit, 1.0, 0.0)
                weight = jnp.where(hit, share, 0.0)
                dm[q, i * slots : (i + 1) * slots] = hot.astype(BF16)
                gm[q, i * slots : (i + 1) * slots] = weight.astype(BF16)

    for c in range(chunks):
        if c == chunks - 1:
            build()
        if c == chunks - 4:
            forward(0)
            own(1)
        if c == chunks - 2:
            hand_over(0)
        shared_step(c)
    last_hop(0)
    hst[0, :tokens] = (silu(acc_g[0, :tokens]) * acc_u[0, :tokens]).astype(BF16)
    pltpu.make_async_copy(hst.at[0, pl.ds(0, tokens)], hs, osem.at[0]).start()
    pltpu.make_async_copy(gm, gt, osem.at[1]).start()
    load(0)
    wait(hs, osem.at[0])

    def dispatch(c):
        slot = lax.rem(c, 2)
        wait(xv.at[slot], ldsem.at[slot])
        for q in range(n):
            v = mm(dm[q], xv[slot, q // chips, q % chips]).astype(BF16)
            for i in range(local):
                z[i, q * slots : (q + 1) * slots] = v[i * slots : (i + 1) * slots]

    @pl.loop(0, chunks - 1)
    def _(c):
        forward(c + 1)

        @pl.when(c + 2 < chunks)
        def _():
            own(c + 2)

        start, groups = 0, (local - 2, 1, 1)
        for i, size in enumerate(groups):
            group = range(start, start + size)
            start += size
            if i == 1:
                hand_over(c + 1)
                last_hop(c + 1)
            if i == 2:
                load(c + 1)
            for e in group:
                wait(wbuf.at[e], wsem.at[e])
            if i == 0:
                for e in range(local - 2, local):
                    fetch_at(c, e)
                dispatch(c)
            if i == 1:
                for e in range(local - 2):
                    fetch_at(c + 1, e)
            for e in group:
                for lo, hi in tiles:
                    for k, acc in ((0, acc_g), (1, acc_u)):
                        v = mm(z[e], wbuf[e, k, :, lo:hi])
                        acc[e, :, lo:hi] = jnp.where(c == 0, 0.0, acc[e, :, lo:hi]) + v

    for e in range(local - 2, local):
        fetch_at(chunks - 1, e)
    dispatch(jnp.int32(chunks - 1))

    for e in range(local):
        slot, to = e, e % 2
        wait(wbuf.at[slot], wsem.at[slot])
        if e >= 2:
            wait(hst.at[to], osem.at[2 + to])
        for lo, hi in tiles:
            g = acc_g[e, :, lo:hi] + mm(z[e], wbuf[slot, 0, :, lo:hi])
            u = acc_u[e, :, lo:hi] + mm(z[e], wbuf[slot, 1, :, lo:hi])
            hst[to, :, lo:hi] = (silu(g) * u).astype(BF16)
        pltpu.make_async_copy(hst.at[to], h.at[e], osem.at[2 + to]).start()

    for to in range(2):
        wait(hst.at[to], osem.at[2 + to])
    wait(gm, osem.at[1])
    for i in range(3):
        wait(x, own_send.at[i])
        wait(x, pass_send.at[i])
    for i in range(2):
        wait(x.at[pl.ds(0, half)], fwd_send.at[i])
    for r in range(1, n):
        wait(meta.at[mine], meta_send.at[r])


def up(n, slots, x, expert, slot, gate, wg, wu, sg, su):
    tokens, d = x.shape
    local, _, ff = wg.shape
    chunks, rows, chips = d // WIDTH, n * slots, n // 2
    dma = pltpu.SemaphoreType.DMA
    flops = 2 * (rows * local + tokens) * d * ff * 2
    moved = 2 * (2 * local + 2) * d * ff
    return pl.pallas_call(
        functools.partial(up_kernel, n, local, slots),
        out_shape=[
            jax.ShapeDtypeStruct((local, rows, ff), BF16),
            jax.ShapeDtypeStruct((tokens, ff), BF16),
            jax.ShapeDtypeStruct((n, local * slots, tokens), BF16),
            jax.ShapeDtypeStruct((chunks, 2, chips, tokens, WIDTH), BF16),
        ],
        in_specs=[ANY, VM, VM, VM, ANY, ANY, ANY, ANY],
        out_specs=[ANY] * 4,
        scratch_shapes=[
            pltpu.VMEM((local, rows, ff), F32),
            pltpu.VMEM((local, rows, ff), F32),
            pltpu.VMEM((local, 2, WIDTH, ff), BF16),
            pltpu.VMEM((2, 2, chips, tokens, WIDTH), BF16),
            pltpu.VMEM((local, rows, WIDTH), BF16),
            pltpu.VMEM((n, local * slots, tokens), BF16),
            pltpu.VMEM((n, local * slots, tokens), BF16),
            pltpu.VMEM((n, 4 * expert.shape[0], tokens), BF16),
            pltpu.VMEM((2, rows, ff), BF16),
            dma((n,)), dma((n,)), dma((3,)), dma((2,)), dma((3,)),
            dma((chunks, 2)), dma((chunks, 2)), dma((chunks,)), dma((chunks,)), dma((chunks,)),
            dma((local,)), dma((chunks,)), dma((2,)), dma((4,)),
        ],
        compiler_params=pltpu.CompilerParams(
            collective_id=0, has_side_effects=True, vmem_limit_bytes=66 * 10**6
        ),
        cost_estimate=pl.CostEstimate(flops=flops, bytes_accessed=moved, transcendentals=0),
    )(x, expert, slot, gate, wg, wu, sg, su)


def down_kernel(n, local, slots, h, hs, gt, wd, sd, y, hv, hsv, gm, wbuf, outs, part, sh, pair_s, pair_r, hop_s, hop_r,
                end_s, end_r, ys, insem, wsem, pair_ss, pair_rs, hop_ss, hop_rs, end_ss, end_rs, ysem):
    me, chips, chip, core, right, left, across = places(n)
    dev_r, dev_l, dev_p = right * 2 + core, left * 2 + core, chip * 2 + 1 - core
    tokens, ff = hs.shape
    chunks = wd.shape[2] // DOWN
    half = tokens // 2
    per = local + 1
    steps = chunks * per

    def cols(c):
        return pl.ds(pl.multiple_of(c * DOWN, DOWN), DOWN)

    def fetch(t):
        slot = lax.rem(t, RING)
        c, e = lax.div(t, per), lax.rem(t, per)

        @pl.when(e < local)
        def _():
            pltpu.make_async_copy(wd.at[e, :, cols(c)], wbuf.at[slot], wsem.at[slot]).start()

        @pl.when(e == local)
        def _():
            pltpu.make_async_copy(sd.at[:, cols(c)], wbuf.at[slot], wsem.at[slot]).start()

    for e in range(local):
        pltpu.make_async_copy(h.at[e], hv.at[e], insem.at[e]).start()
        if e < 2:
            fetch(jnp.int32(e))
    pltpu.make_async_copy(hs, hsv, insem.at[local]).start()
    pltpu.make_async_copy(gt, gm, insem.at[local + 1]).start()

    barrier = pltpu.get_barrier_semaphore()
    for dev in (dev_r, dev_l, dev_p):
        pl.semaphore_signal(barrier, inc=1, device_id={"ep": dev}, device_id_type=MESH)
    pl.semaphore_wait(barrier, 3)

    def first_hop(c):
        k, b = lax.rem(c, 3), lax.rem(c, 2)

        @pl.when(c >= 2)
        def _():
            for i in range(2):
                wait(hop_s.at[b, i], hop_ss.at[b, i])

        wait(pair_r.at[c], pair_rs.at[c])
        v = (part[k, across] + pair_r[c, across].astype(F32)).astype(BF16)
        hop_s[b, 0] = v[:half]
        hop_s[b, 1] = v[half:]
        send(hop_s.at[b, 0], hop_r.at[c, 0], hop_ss.at[b, 0], hop_rs.at[c, 0], dev_r)
        send(hop_s.at[b, 1], hop_r.at[c, 1], hop_ss.at[b, 1], hop_rs.at[c, 1], dev_l)

    def second_hop(c):
        k, b = lax.rem(c, 3), lax.rem(c, 2)

        @pl.when(c >= 2)
        def _():
            for i in range(2):
                wait(end_s.at[b, i], end_ss.at[b, i])

        up, lo = pl.ds(0, half), pl.ds(half, half)
        for i, to in ((0, right), (1, left)):
            wait(hop_r.at[c, i], hop_rs.at[c, i])
            rows, others = (up, lo) if i == 0 else (lo, up)
            v = part[k, to, rows] + pair_r[c, to, rows].astype(F32) + hop_r[c, i].astype(F32)
            end_s[b, i, rows] = v.astype(BF16)
            v = part[k, to, others] + pair_r[c, to, others].astype(F32)
            end_s[b, i, others] = v.astype(BF16)
            send(end_s.at[b, i], end_r.at[c, i], end_ss.at[b, i], end_rs.at[c, i], (dev_r, dev_l)[i])

    def finish(c):
        k, b = lax.rem(c, 3), lax.rem(c, 2)

        @pl.when(c >= 2)
        def _():
            wait(ys.at[b], ysem.at[b])

        for i in range(2):
            wait(end_r.at[c, i], end_rs.at[c, i])
        v = part[k, chip] + pair_r[c, chip].astype(F32) + end_r[c, 0].astype(F32) + end_r[c, 1].astype(F32)
        ys[b] = (v + sh[k]).astype(BF16)
        pltpu.make_async_copy(ys.at[b], y.at[:, cols(c)], ysem.at[b]).start()

    @pl.loop(0, steps)
    def _(t):
        c, e = lax.div(t, per), lax.rem(t, per)
        slot = lax.rem(t, RING)

        @pl.when((e == 1) & (c >= 1))
        def _():
            first_hop(c - 1)

        @pl.when((e == 2) & (c >= 2))
        def _():
            second_hop(c - 2)

        @pl.when((e == 4) & (c >= 3))
        def _():
            finish(c - 3)

        @pl.when((c == 0) & (e < local))
        def _():
            wait(hv.at[e], insem.at[e])

        @pl.when(t == local)
        def _():
            wait(hs, insem.at[local])
            wait(gt, insem.at[local + 1])

        wait(wbuf.at[slot], wsem.at[slot])

        @pl.when(t + 2 < steps)
        def _():
            fetch(t + 2)

        @pl.when(e < local)
        def _():
            v = mm(hv[e], wbuf[slot]).astype(BF16)
            for q in range(n):
                outs[q, pl.ds(pl.multiple_of(e * slots, slots), slots)] = v[q * slots : (q + 1) * slots]

        @pl.when(e == local)
        def _():
            b, k = lax.rem(c, 2), lax.rem(c, 3)

            @pl.when(c >= 2)
            def _():
                wait(pair_s.at[b], pair_ss.at[b])

            def combined(q):
                return lax.dot_general(gm[q], outs[q], (((0,), (0,)), ((), ())), preferred_element_type=F32)

            for i in range(chips):
                pair_s[b, i] = combined((1 - core) * chips + i).astype(BF16)
            send(pair_s.at[b], pair_r.at[c], pair_ss.at[b], pair_rs.at[c], dev_p)
            for i in range(chips):
                part[k, i] = combined(core * chips + i)
            sh[k] = mm(hsv[...], wbuf[slot])

    end = chunks - 1
    second_hop(jnp.int32(end - 1))
    first_hop(jnp.int32(end))
    finish(jnp.int32(end - 2))
    second_hop(jnp.int32(end))
    finish(jnp.int32(end - 1))
    finish(jnp.int32(end))
    for b in range(2):
        wait(pair_s.at[b], pair_ss.at[b])
        wait(ys.at[b], ysem.at[b])
        for i in range(2):
            wait(hop_s.at[b, i], hop_ss.at[b, i])
            wait(end_s.at[b, i], end_ss.at[b, i])


def down(n, slots, h, hs, gt, wd, sd):
    local, rows, ff = h.shape
    tokens, d = hs.shape[0], wd.shape[2]
    chunks, chips, half = d // DOWN, n // 2, tokens // 2
    dma = pltpu.SemaphoreType.DMA
    flops = 2 * (rows * local + tokens) * d * ff
    return pl.pallas_call(
        functools.partial(down_kernel, n, local, slots),
        out_shape=jax.ShapeDtypeStruct((tokens, d), BF16),
        in_specs=[ANY] * 5,
        out_specs=ANY,
        scratch_shapes=[
            pltpu.VMEM(h.shape, BF16),
            pltpu.VMEM(hs.shape, BF16),
            pltpu.VMEM(gt.shape, BF16),
            pltpu.VMEM((RING, ff, DOWN), BF16),
            pltpu.VMEM((n, local * slots, DOWN), BF16),
            pltpu.VMEM((3, chips, tokens, DOWN), F32),
            pltpu.VMEM((3, tokens, DOWN), F32),
            pltpu.VMEM((2, chips, tokens, DOWN), BF16),
            pltpu.VMEM((chunks, chips, tokens, DOWN), BF16),
            pltpu.VMEM((2, 2, half, DOWN), BF16),
            pltpu.VMEM((chunks, 2, half, DOWN), BF16),
            pltpu.VMEM((2, 2, tokens, DOWN), BF16),
            pltpu.VMEM((chunks, 2, tokens, DOWN), BF16),
            pltpu.VMEM((2, tokens, DOWN), BF16),
            dma((local + 2,)), dma((RING,)), dma((2,)), dma((chunks,)), dma((2, 2)), dma((chunks, 2)),
            dma((2, 2)), dma((chunks, 2)), dma((2,)),
        ],
        compiler_params=pltpu.CompilerParams(
            collective_id=1, has_side_effects=True, vmem_limit_bytes=62 * 2**20
        ),
        cost_estimate=pl.CostEstimate(flops=flops, bytes_accessed=2 * (local + 1) * d * ff, transcendentals=0),
    )(h, hs, gt, wd, sd)


def solution(mesh):
    n = mesh.shape["ep"]

    def body(x, expert, slot, gate, w_gate, w_up, w_down, s_gate, s_up, s_down):
        x, expert, slot, gate = x[0, 0], expert[0, 0], slot[0, 0], gate[0, 0]
        (tokens, top), local = expert.shape, w_gate.shape[0]
        slots = 5 * tokens * top // (4 * local * n)
        h, hs, gt, _ = up(n, slots, x, expert.T, slot.T, gate.T, w_gate, w_up, s_gate, s_up)
        return down(n, slots, h, hs, gt, w_down, s_down)[None, None]

    a, e, r = P("dp", "ep", None, None), P("ep", None, None), P(None, None)
    return jax.shard_map(body, mesh=mesh, in_specs=(a, a, a, a, e, e, e, r, r, r), out_specs=a, check_vma=False)
```
